32 devices in a mesh: expert: 4 (over z), tensor: 8 (over y, x, core).
Axes of the slice: x: 2, y: 2, z: 4, core: 2. Of those that a mesh axis runs over, the one named last changes fastest.
Arguments:
- expert_inputs: bfloat16 [8, 64, 4096], P('expert'), may hold values from -6 to 6
- gates: float32 [8, 64], P('expert'), may hold values from 0.2 to 1
- chosen_tokens: int32 [8, 64], replicated, may hold values from 0 to 4095, as said below
- w_gate: bfloat16 [8, 4096, 1792], P('expert', None, 'tensor'), may hold values from -0.09375 to 0.09375
- w_up: bfloat16 [8, 4096, 1792], P('expert', None, 'tensor'), may hold values from -0.09375 to 0.09375
- w_down: bfloat16 [8, 1792, 4096], P('expert', 'tensor'), may hold values from -0.125 to 0.125
- residual: bfloat16 [4096, 4096], P(('expert', 'tensor')), may hold values from -6 to 6
- norm_gain: float32 [4096], replicated, may hold values from 0.5 to 1.5
- w_qkv: bfloat16 [4096, 12288], P(None, 'tensor'), may hold values from -0.09375 to 0.09375
Outputs:
- stream: bfloat16 [4096, 4096], P(('expert', 'tensor'))
- projected: bfloat16 [4096, 12288], P('expert', 'tensor')
The draws below stay inside these ranges and needn't reach their ends.
Inputs may be any that keep to these rules, and one draw needn't show every extreme that they name: `chosen_tokens`: each row holds 64 different token indices; at most 4 of a row lie in one block of 128 consecutive tokens, and in every draw some block holds 4 tokens of every row.
All inputs are finite; a program needn't handle non-finite values.
Results may differ from the reference program's by a relative error of at most 0.005.
Values may be sent and summed in bfloat16 or wider, within the bound.
A program may use at most 128 MiB of HBM per device.

```python
import jax
import jax.numpy as jnp
from jax import lax

D = 4096
FF = 1792
TOK_DEV = 128
MOST = 4
EXPERTS_LIVE = 8
CAP = 64
TOKENS = 4096


def draw_chosen_tokens(key, part):
    owner_total = TOKENS // TOK_DEV
    key_hot, key_forced, key_score, key_base = jax.random.split(jax.random.fold_in(key, 17), 4)
    popularity = jax.random.randint(key_hot, (owner_total,), 0, 4)
    mandatory_pick = jax.random.randint(key_forced, (), 0, owner_total)
    holder_numbers = jnp.arange(owner_total, dtype=jnp.int32)
    extra_score = popularity * 16384 + jnp.where(holder_numbers == mandatory_pick, 262144, 0)
    noise_term = jax.random.randint(key_score, (EXPERTS_LIVE, owner_total, MOST), 0, 65536)
    affinity_scores = noise_term + extra_score[None, :, None]
    ticket_ids = jnp.arange(owner_total * MOST, dtype=jnp.int32).reshape(1, owner_total, MOST)
    distinct = (affinity_scores * (owner_total * MOST) + ticket_ids).reshape(EXPERTS_LIVE, owner_total * MOST)
    picked_scores, picked = jax.lax.top_k(distinct, CAP)
    picked_owner = picked // MOST
    picked_rank = picked % MOST
    base_offset = jax.random.randint(key_base, (EXPERTS_LIVE, owner_total), 0, TOK_DEV)
    chosen_base = jnp.take_along_axis(base_offset, picked_owner, axis=1)
    offsets = (chosen_base + picked_rank) % TOK_DEV
    return (picked_owner * TOK_DEV + offsets).astype(jnp.int32)


def level_of(key, shape, shards, smallest, top_value):
    loudness, own = 1.0, jax.random.fold_in(key, 6)
    for axis_at, parts in shards:
        heights = jnp.exp(jax.random.uniform(jax.random.fold_in(own, axis_at), (parts,), jnp.float32, smallest / len(shards), top_value / len(shards)))
        loudness = loudness * jnp.repeat(heights, shape[axis_at] // parts).reshape([-1 if axis == axis_at else 1 for axis in range(len(shape))])
    return loudness


def normal_values(rng, extent, spread, most, cuts=(), held_as=jnp.bfloat16):
    entries = spread * jax.random.normal(rng, extent, jnp.float32)
    if cuts:
        entries = entries * level_of(rng, extent, cuts, -0.22, 0.18)
    return jnp.clip(entries, -most, most).astype(held_as)


def setup_inputs(seed: int = 0) -> dict:
    streams_of = jax.random.split(jax.random.key(seed), 10)
    expert_inputs = normal_values(streams_of[0], (EXPERTS_LIVE, CAP, D), 1.0, 6.0, ((0, 4),))
    gates = jnp.clip(0.2 + 0.8 * jax.random.uniform(streams_of[1], (EXPERTS_LIVE, CAP), jnp.float32) ** level_of(streams_of[1], (EXPERTS_LIVE, CAP), ((0, 4),), -0.2, 0.2), 0.2, 1.0)
    chosen_tokens = draw_chosen_tokens(jax.random.fold_in(streams_of[9], 71), 0)
    w_gate = normal_values(streams_of[3], (EXPERTS_LIVE, D, FF), D ** -0.5, 0.09375, ((0, 4), (2, 8)))
    w_up = normal_values(streams_of[4], (EXPERTS_LIVE, D, FF), D ** -0.5, 0.09375, ((0, 4), (2, 8)))
    w_down = normal_values(streams_of[5], (EXPERTS_LIVE, FF, D), FF ** -0.5, 0.125, ((0, 4), (1, 8)))
    residual = normal_values(streams_of[6], (TOKENS, D), 1.0, 6.0, ((0, 32),))
    norm_gain = jnp.clip(1.0 + 0.1 * jax.random.normal(streams_of[7], (D,), jnp.float32), 0.5, 1.5)
    w_qkv = normal_values(streams_of[8], (D, 3 * D), D ** -0.5, 0.09375, ((1, 8),))
    return {"expert_inputs": expert_inputs, "gates": gates, "chosen_tokens": chosen_tokens, "w_gate": w_gate, "w_up": w_up, "w_down": w_down, "residual": residual, "norm_gain": norm_gain, "w_qkv": w_qkv}


def expert_apply(operands):
    inputs_block, gate_block, gate_weight, up_weight, down_weight = operands
    gate_part = jnp.dot(inputs_block, gate_weight, preferred_element_type=jnp.float32)
    up_part = jnp.dot(inputs_block, up_weight, preferred_element_type=jnp.float32)
    hidden = (jax.nn.silu(gate_part) * up_part).astype(jnp.bfloat16)
    return jnp.dot(hidden, down_weight, preferred_element_type=jnp.float32) * gate_block[:, None]

def reference(expert_inputs, gates, chosen_tokens, w_gate, w_up, w_down, residual, norm_gain, w_qkv):
    expert_out = lax.map(expert_apply, (expert_inputs, gates, w_gate, w_up, w_down))
    scattered = jnp.zeros((TOKENS, D), jnp.float32).at[chosen_tokens.reshape(-1)].add(expert_out.reshape(-1, D))
    combined = residual.astype(jnp.float32) + scattered
    stream = combined.astype(jnp.bfloat16)
    scale_rows = lax.rsqrt(lax.optimization_barrier(jnp.mean(combined * combined, axis=-1, keepdims=True)) + 1e-06)
    normed = (combined * scale_rows * norm_gain[None, :]).astype(jnp.bfloat16)
    projected = jnp.dot(normed, w_qkv, preferred_element_type=jnp.float32).astype(jnp.bfloat16)
    return (stream, projected)
```

```python
import functools

import jax
import jax.numpy as jnp
from jax import lax
from jax.experimental import pallas as pl
from jax.experimental.pallas import tpu as pltpu
from jax.sharding import PartitionSpec as P

MOST = 4
MESH = pl.DeviceIdType.MESH


def finish_kernel(
    row_steps,
    order,
    owner_ref,
    slots_ref,
    residual_ref,
    rows_ref,
    gain_ref,
    weight_ref,
    stream_ref,
    projected_ref,
    combined_ref,
    normed_ref,
):
    step = pl.program_id(0)
    tok_rows, feature_width = residual_ref.shape
    chunk = rows_ref.shape[2]

    @pl.when(step < row_steps)
    def _():
        tokens = lax.broadcasted_iota(jnp.int32, (tok_rows, slots_ref.shape[1]), 0)
        placement = jnp.where(slots_ref[...] == tokens + step * tok_rows, 1.0, 0.0).astype(
            jnp.bfloat16
        )
        squares = jnp.zeros((tok_rows, 128), jnp.float32)
        for place, start in enumerate(range(0, feature_width, chunk)):
            cols = pl.ds(start, chunk)
            combined = residual_ref[:, cols].astype(jnp.float32) + jnp.dot(
                placement, rows_ref[order[place]], preferred_element_type=jnp.float32
            )
            combined_ref[:, cols] = combined
            for part in range(0, chunk, 128):
                piece = combined[:, part : part + 128]
                squares = squares + piece * piece
        mean = jnp.sum(squares, axis=1, keepdims=True) / feature_width
        scale = lax.rsqrt(mean + 1e-06)
        begin = pl.multiple_of(step * tok_rows, tok_rows)
        for start in range(0, feature_width, chunk):
            cols = pl.ds(start, chunk)
            normed_ref[pl.ds(begin, tok_rows), cols] = (
                combined_ref[:, cols] * scale * gain_ref[:, cols]
            ).astype(jnp.bfloat16)

        @pl.when(step == owner_ref[0])
        def _():
            stream_ref[...] = combined_ref[...].astype(jnp.bfloat16)

    @pl.when(step >= row_steps)
    def _():
        projected_ref[...] = jnp.dot(
            normed_ref[...], weight_ref[...], preferred_element_type=jnp.float32
        ).astype(jnp.bfloat16)


def finish(owner, slots, residual_all, rows, order, gain, w_qkv, tok_rows):
    total_rows, feature_width = residual_all.shape
    columns = w_qkv.shape[1]
    tile = 256
    row_steps = total_rows // tok_rows
    col_steps = columns // tile
    slot_total = rows.shape[1]
    return pl.pallas_call(
        functools.partial(finish_kernel, row_steps, order),
        grid=(row_steps + col_steps,),
        in_specs=[
            pl.BlockSpec(memory_space=pltpu.SMEM),
            pl.BlockSpec((1, slot_total), lambda i: (0, 0)),
            pl.BlockSpec((tok_rows, feature_width), lambda i: (jnp.minimum(i, row_steps - 1), 0)),
            pl.BlockSpec(rows.shape, lambda i: (0, 0, 0)),
            pl.BlockSpec((1, feature_width), lambda i: (0, 0)),
            pl.BlockSpec((feature_width, tile), lambda i: (0, jnp.maximum(i - row_steps, 0))),
        ],
        out_specs=[
            pl.BlockSpec((tok_rows, feature_width), lambda i: (0, 0)),
            pl.BlockSpec((total_rows, tile), lambda i: (0, jnp.maximum(i - row_steps, 0))),
        ],
        out_shape=[
            jax.ShapeDtypeStruct((tok_rows, feature_width), jnp.bfloat16),
            jax.ShapeDtypeStruct((total_rows, columns), jnp.bfloat16),
        ],
        scratch_shapes=[
            pltpu.VMEM((tok_rows, feature_width), jnp.float32),
            pltpu.VMEM((total_rows, feature_width), jnp.bfloat16),
        ],
        compiler_params=pltpu.CompilerParams(
            vmem_limit_bytes=60 * 1024 * 1024, dimension_semantics=("arbitrary",)
        ),
        cost_estimate=pl.CostEstimate(
            flops=2 * total_rows * feature_width * (columns + slot_total),
            bytes_accessed=2 * (feature_width * columns + total_rows * columns),
            transcendentals=0,
        ),
    )(owner, slots, residual_all, rows, gain, w_qkv)


def comm_kernel(
    groups,
    keep,
    inputs_hbm,
    gates_hbm,
    tokens_hbm,
    gain_hbm,
    gate_hbm,
    up_hbm,
    down_hbm,
    residual_hbm,
    weight_hbm,
    stream_ref,
    projected_ref,
    inputs,
    gates,
    tokens,
    gain,
    gate_w,
    up_w,
    down_w,
    raw,
    weight,
    blocks,
    rows,
    acc,
    row_acc,
    row_out,
    ranks,
    slot_col,
    slots,
    scales,
    partial,
    half_in,
    chips_sum,
    chips_in,
    outgoing,
    load_sem,
    expert_sem,
    first_send,
    first_recv,
    reduce_send,
    reduce_recv,
    group_send,
    group_recv,
    link_send,
    link_recv,
    pair_send,
    pair_recv,
    row_send,
    row_recv,
    scale_send,
    scale_recv,
):
    group = lax.axis_index("expert")
    me = lax.axis_index("tensor")
    core = me % 2
    partner = me + 1 - 2 * core
    along_x = me + 2 - 4 * ((me // 2) % 2)
    along_y = me + 4 - 8 * (me // 4)
    across = along_x + 4 - 8 * (me // 4)
    local_experts, slot_count, feature_width = inputs.shape
    chips, row_total, width = chips_sum.shape
    members, units, tok_rows, _ = blocks.shape
    pair = 2 * tok_rows
    half_units = units // 2
    group_rows = members * tok_rows
    slot_total = slots.shape[1]
    tile = 512
    col_tiles = weight.shape[1] // tile
    f32, bf16 = jnp.float32, jnp.bfloat16

    def load(source, target, sem):
        copy = pltpu.make_async_copy(source, target, sem)
        copy.start()
        return copy

    load_tokens = load(tokens_hbm, tokens, load_sem.at[0])
    load_gates = load(gates_hbm, gates, load_sem.at[1])
    load_gain = load(gain_hbm, gain, load_sem.at[2])
    load_raw = load(residual_hbm, raw, load_sem.at[3])
    load_inputs = load(inputs_hbm, inputs, load_sem.at[4])
    load_experts = [
        [
            load(hbm.at[expert], vmem.at[expert], expert_sem.at[3 * expert + index])
            for index, (hbm, vmem) in enumerate(
                ((gate_hbm, gate_w), (up_hbm, up_w), (down_hbm, down_w))
            )
        ]
        for expert in range(local_experts)
    ]
    load_weight = load(weight_hbm, weight, load_sem.at[5])

    barrier = pltpu.get_barrier_semaphore()
    peers = [(group, lax.rem(me + d, members)) for d in range(1, members)]
    peers += [((group + d) % groups, me) for d in range(1, groups)]
    for device in peers:
        pl.semaphore_signal(barrier, inc=1, device_id=device, device_id_type=MESH)

    sent = []

    def send(source, target, send_sem, recv_sem, device):
        copy = pltpu.make_async_remote_copy(
            src_ref=source,
            dst_ref=target,
            send_sem=send_sem,
            recv_sem=recv_sem,
            device_id=(group, device),
            device_id_type=MESH,
        )
        copy.start()
        sent.append(copy)
        return copy

    def on_link(index, origin, unit, device):
        part = blocks.at[origin, unit]
        return send(part, part, link_send.at[index], link_recv.at[index], device)

    def own_x(unit):
        return on_link(unit, me, unit, along_x)

    def own_y(unit):
        return on_link(units + unit, me, unit, along_y)

    def relay(unit):
        if unit < half_units:
            return on_link(2 * units + unit, along_x, unit, along_y)
        return on_link(2 * units + unit, along_y, unit, along_x)

    def to_partner(role, unit):
        part = blocks.at[(along_x, along_y, across)[role], unit]
        index = role * units + unit
        return send(part, part, pair_send.at[index], pair_recv.at[index], partner)

    def rows_to(index, origin, start, size, device):
        part = rows.at[origin, pl.ds(start, size)]
        return send(part, part, row_send.at[index], row_recv.at[index], device)

    def eye(size):
        shape = (size, size)
        return lax.broadcasted_iota(jnp.int32, shape, 0) == lax.broadcasted_iota(
            jnp.int32, shape, 1
        )

    def column(row):
        return jnp.sum(jnp.where(eye(row.shape[1]), row, 0.0), axis=1, keepdims=True)

    load_tokens.wait()
    order = lax.broadcasted_iota(jnp.int32, (slot_count, slot_count), 0)
    later = lax.broadcasted_iota(jnp.int32, (slot_count, slot_count), 1)
    before = jnp.where(order < later, 1.0, 0.0).astype(bf16)
    chosen = tokens[...]
    for place in range(groups):
        inside = (chosen >= place * group_rows) & (chosen < (place + 1) * group_rows)
        taken = jnp.where(inside, 1.0, 0.0)
        rank = jnp.dot(taken.astype(bf16), before, preferred_element_type=f32)
        ranks[place] = jnp.where(inside, rank, -1.0)
    kept = lax.broadcasted_iota(jnp.int32, (keep, slot_count), 0).astype(f32)
    mine = ranks[group]
    local = (chosen - group * group_rows + 1).astype(f32)
    for expert in range(chosen.shape[0]):
        hit = mine[expert : expert + 1, :] == kept
        slot_col[expert * keep : (expert + 1) * keep, :] = jnp.sum(
            jnp.where(hit, local[expert : expert + 1, :], 0.0), axis=1, keepdims=True
        )
    slots[...] = (
        jnp.sum(jnp.where(eye(slot_total), slot_col[...], 0.0), axis=0, keepdims=True) - 1.0
    )

    load_gain.wait()
    load_raw.wait()
    for unit in range(units):
        cols = pl.ds(unit * width, width)
        blocks[me, unit] = (raw[:, cols].astype(f32) * gain[:, cols]).astype(bf16)

    pl.semaphore_wait(barrier, len(peers))

    x0, y4 = own_x(0), own_y(half_units)
    x1, y5 = own_x(1), own_y(half_units + 1)
    part = blocks.at[me]
    pair_own = send(part, part, pair_send.at[3 * units], pair_recv.at[3 * units], partner)

    load_gates.wait()
    load_inputs.wait()
    contract = (((1,), (1,)), ((), ()))
    firsts = []
    for expert in range(local_experts):
        for copy in load_experts[expert]:
            copy.wait()
        gate_part = lax.dot_general(
            inputs[expert], gate_w[expert], contract, preferred_element_type=f32
        )
        up_part = lax.dot_general(
            inputs[expert], up_w[expert], contract, preferred_element_type=f32
        )
        hidden = (gate_part / (1.0 + jnp.exp(-gate_part)) * up_part).astype(bf16)
        scale_by = column(gates[expert : expert + 1, :])
        lines = pl.ds(expert * slot_count, slot_count)
        for place in range(2 * chips):
            value = jnp.dot(
                hidden,
                down_w[expert, :, place * width : (place + 1) * width],
                preferred_element_type=f32,
            )
            partial[place, lines, :] = (value * scale_by).astype(bf16)
        firsts.append(
            send(
                partial.at[pl.ds((1 - core) * chips, chips), lines],
                half_in.at[:, lines],
                first_send.at[expert],
                first_recv.at[expert],
                partner,
            )
        )

    for expert, copy in enumerate(firsts):
        copy.wait_recv()
        lines = pl.ds(expert * slot_count, slot_count)
        for chip in range(chips):
            chips_sum[chip, lines, :] = (
                partial[core * chips + chip, lines, :].astype(f32)
                + half_in[chip, lines, :].astype(f32)
            ).astype(bf16)
    reduces = [
        send(
            chips_sum.at[device // 2],
            chips_in.at[index],
            reduce_send.at[index],
            reduce_recv.at[index],
            device,
        )
        for index, device in enumerate((across, along_x, along_y))
    ]
    x2, y6 = own_x(2), own_y(half_units + 2)
    x3, y7 = own_x(3), own_y(half_units + 3)

    def accumulate(chip, unit):
        lines = pl.ds(pl.multiple_of(unit * width, width), width)
        left = blocks[pl.ds(2 * chip, 2), unit].reshape(pair, width)
        for index in range(col_tiles):
            cols = pl.ds(index * tile, tile)
            acc[chip, :, cols] += jnp.dot(left, weight[lines, cols], preferred_element_type=f32)

    def clear(chip, carry):
        acc[chip] = jnp.zeros(acc.shape[1:], f32)
        return carry

    lax.fori_loop(0, chips, clear, 0)
    row_acc[...] = jnp.zeros(row_acc.shape, f32)

    chip_own, chip_x, chip_y, chip_a = me // 2, along_x // 2, along_y // 2, across // 2

    def each(start, size, body):
        def step(index, carry):
            body(index)
            return carry

        lax.fori_loop(start, start + size, step, 0)

    def own(index):
        accumulate(chip_own, index)
        accumulate(chip_own, index + half_units)

    def near(index):
        accumulate(chip_x, index)
        accumulate(chip_y, index + half_units)

    def late(index):
        accumulate(chip_x, index + half_units)
        accumulate(chip_y, index)

    def far(index):
        accumulate(chip_a, index)
        accumulate(chip_a, index + half_units)

    pair_own.wait_recv()
    load_weight.wait()
    each(0, half_units, own)

    x0.wait_recv()
    px0 = to_partner(0, 0)
    y4.wait_recv()
    py4 = to_partner(1, half_units)
    a0, a4 = relay(0), relay(half_units)
    x1.wait_recv()
    px1 = to_partner(0, 1)
    y5.wait_recv()
    py5 = to_partner(1, half_units + 1)
    a1, a5 = relay(1), relay(half_units + 1)

    for copy in reduces:
        copy.wait_recv()
    total = chips_sum[me // 2].astype(f32)
    for index in range(3):
        total = total + chips_in[index].astype(f32)
    total = total.astype(bf16)
    for place in range(groups):
        for expert in range(local_experts):
            rank = ranks[place, pl.ds(group * local_experts + expert, 1), :]
            table = jnp.where(rank == kept, 1.0, 0.0).astype(bf16)
            outgoing[place, expert * keep : (expert + 1) * keep, :] = jnp.dot(
                table,
                total[expert * slot_count : (expert + 1) * slot_count],
                preferred_element_type=f32,
            ).astype(bf16)
    exchanges = []
    for d in range(1, groups):
        copy = pltpu.make_async_remote_copy(
            src_ref=outgoing.at[(group + d) % groups],
            dst_ref=rows.at[me, group],
            send_sem=group_send.at[d - 1],
            recv_sem=group_recv.at[d - 1],
            device_id=((group + d) % groups, me),
            device_id_type=MESH,
        )
        copy.start()
        exchanges.append(copy)
    rows[me, group] = outgoing[group]

    for copy in (px0, py4, px1, py5):
        copy.wait_recv()
    each(0, 2, near)
    x2.wait_recv()
    px2 = to_partner(0, 2)
    y6.wait_recv()
    py6 = to_partner(1, half_units + 2)

    for copy in exchanges:
        copy.wait_recv()
    groups_half = groups // 2
    rest = groups - groups_half
    row_x, row_y = rows_to(0, me, 0, groups, along_x), rows_to(1, me, 0, groups, along_y)
    row_own = rows_to(4, me, 0, groups, partner)

    x3.wait_recv()
    px3 = to_partner(0, 3)
    y7.wait_recv()
    py7 = to_partner(1, half_units + 3)
    for copy in (px2, py6, px3, py7):
        copy.wait_recv()
    each(2, 2, near)
    a0.wait_recv()
    pa0 = to_partner(2, 0)
    a4.wait_recv()
    pa4 = to_partner(2, half_units)

    row_x.wait_recv()
    row_ox = rows_to(2, along_x, 0, groups_half, along_y)
    row_px = rows_to(5, along_x, 0, groups, partner)
    row_y.wait_recv()
    row_oy = rows_to(3, along_y, groups_half, rest, along_x)
    row_py = rows_to(6, along_y, 0, groups, partner)
    a2, a6 = relay(2), relay(half_units + 2)
    a3, a7 = relay(3), relay(half_units + 3)
    last = [(own_x(half_units + step), own_y(step)) for step in range(half_units - 2)]

    a1.wait_recv()
    pa1 = to_partner(2, 1)
    a5.wait_recv()
    pa5 = to_partner(2, half_units + 1)
    for copy in (pa0, pa4, pa1, pa5):
        copy.wait_recv()
    each(0, 2, far)

    row_ox.wait_recv()
    row_oy.wait_recv()
    row_pa = rows_to(7, across, 0, groups, partner)
    for copy in (row_own, row_px, row_py, row_pa):
        copy.wait_recv()

    def placement(begin, size):
        line = lax.broadcasted_iota(jnp.int32, (size, slot_total), 0) + begin
        return jnp.where(slots[...] == line.astype(f32), 1.0, 0.0).astype(bf16)

    own_place = placement(me * tok_rows, tok_rows)

    def combine(source, squares):
        start = ((source % 2) * chips + source // 2) * width
        cols = pl.ds(pl.multiple_of(start, width), width)
        values = rows[source].reshape(slot_total, width)
        combined = raw[:, cols].astype(f32) + jnp.dot(
            own_place, values, preferred_element_type=f32
        )
        stream_ref[:, cols] = combined.astype(bf16)
        for piece in range(0, width, 128):
            value = combined[:, piece : piece + 128]
            squares = squares + value * value
        return squares

    squares = lax.fori_loop(0, members, combine, jnp.zeros((tok_rows, 128), f32))
    scale = lax.rsqrt(jnp.sum(squares, axis=1, keepdims=True) / feature_width + 1e-06)
    scale_row = jnp.sum(jnp.where(eye(tok_rows), scale, 0.0), axis=0, keepdims=True)
    scales[me] = jnp.broadcast_to(scale_row, scales.shape[1:])
    part = scales.at[me]
    scalings = [
        send(
            part, part, scale_send.at[d - 1], scale_recv.at[d - 1], lax.rem(me + d, members)
        )
        for d in range(1, members)
    ]
    last += [
        (own_x(half_units + step), own_y(step)) for step in range(half_units - 2, half_units)
    ]

    a2.wait_recv()
    pa2 = to_partner(2, 2)
    a6.wait_recv()
    pa6 = to_partner(2, half_units + 2)

    def multiply_rows(source):
        start = ((source % 2) * chips + source // 2) * width
        lines = pl.ds(pl.multiple_of(start, width), width)
        values = rows[source].reshape(slot_total, width).astype(f32)
        values = (values * gain[:, lines]).astype(bf16)
        for index in range(col_tiles):
            cols = pl.ds(index * tile, tile)
            row_acc[:, cols] += jnp.dot(values, weight[lines, cols], preferred_element_type=f32)

    each(0, members, multiply_rows)
    row_out[...] = row_acc[...].astype(bf16)

    def place_rows(chip):
        spread = placement(chip * pair, pair)
        for index in range(col_tiles):
            cols = pl.ds(index * tile, tile)
            acc[chip, :, cols] += jnp.dot(spread, row_out[:, cols], preferred_element_type=f32)

    each(0, chips, place_rows)

    a3.wait_recv()
    pa3 = to_partner(2, 3)
    a7.wait_recv()
    pa7 = to_partner(2, half_units + 3)
    for copy in (pa2, pa6, pa3, pa7):
        copy.wait_recv()
    each(2, 2, far)

    def finish(chip):
        def body(side, carry):
            scale_by = column(scales[2 * chip + side, 0:1, :])
            lines = pl.ds(pl.multiple_of(side * tok_rows, tok_rows), tok_rows)
            begin = pl.multiple_of(chip * pair + side * tok_rows, tok_rows)
            projected_ref[pl.ds(begin, tok_rows), :] = (acc[chip, lines, :] * scale_by).astype(
                bf16
            )
            return carry

        lax.fori_loop(0, 2, body, 0)

    drain = len(sent) - 2 * half_units
    passed = []
    for step, (near_x, near_y) in enumerate(last):
        near_x.wait_recv()
        px = to_partner(0, half_units + step)
        near_y.wait_recv()
        py = to_partner(1, step)
        passed.append((px, py))
        if step:
            for copy in passed[step - 1]:
                copy.wait_recv()
            each(step - 1, 1, late)
        if step == half_units - 2:
            for copy in scalings:
                copy.wait_recv()
            finish(chip_own)
            finish(chip_a)
            for copy in sent[:drain] + exchanges:
                copy.wait_send()
    for copy in passed[-1]:
        copy.wait_recv()
    each(half_units - 1, 1, late)
    finish(chip_x)
    finish(chip_y)

    for copy in sent[drain:]:
        copy.wait_send()


def communicate(
    groups, members, keep, inputs, gates, tokens, w_gate, w_up, w_down, residual, gain, w_qkv
):
    local_experts, slot_count, feature_width = inputs.shape
    tok_rows = residual.shape[0]
    row_total = local_experts * slot_count
    width = feature_width // members
    chips = members // 2
    columns = w_qkv.shape[1]
    slot_total = tokens.shape[0] * keep
    bf16, f32 = jnp.bfloat16, jnp.float32
    hbm = pl.BlockSpec(memory_space=pltpu.HBM)
    vmem = pl.BlockSpec(memory_space=pltpu.VMEM)
    dma = pltpu.SemaphoreType.DMA
    gate_t, up_t = jnp.swapaxes(w_gate, 1, 2), jnp.swapaxes(w_up, 1, 2)
    return pl.pallas_call(
        functools.partial(comm_kernel, groups, keep),
        in_specs=[hbm] * 9,
        out_specs=[vmem, vmem],
        out_shape=[
            pltpu.VMEM((tok_rows, feature_width), bf16),
            pltpu.VMEM((members * tok_rows, columns), bf16),
        ],
        scratch_shapes=[
            pltpu.VMEM(inputs.shape, bf16),
            pltpu.VMEM(gates.shape, f32),
            pltpu.VMEM(tokens.shape, jnp.int32),
            pltpu.VMEM(gain.shape, f32),
            pltpu.VMEM(gate_t.shape, bf16),
            pltpu.VMEM(up_t.shape, bf16),
            pltpu.VMEM(w_down.shape, bf16),
            pltpu.VMEM(residual.shape, bf16),
            pltpu.VMEM(w_qkv.shape, bf16),
            pltpu.VMEM((members, members, tok_rows, width), bf16),
            pltpu.VMEM((members, groups, local_experts * keep, width), bf16),
            pltpu.VMEM((chips, 2 * tok_rows, columns), f32),
            pltpu.VMEM((slot_total, columns), f32),
            pltpu.VMEM((slot_total, columns), bf16),
            pltpu.VMEM((groups,) + tokens.shape, f32),
            pltpu.VMEM((slot_total, 1), f32),
            pltpu.VMEM((1, slot_total), f32),
            pltpu.VMEM((members, 8, tok_rows), f32),
            pltpu.VMEM((members, row_total, width), bf16),
            pltpu.VMEM((chips, row_total, width), bf16),
            pltpu.VMEM((chips, row_total, width), bf16),
            pltpu.VMEM((chips - 1, row_total, width), bf16),
            pltpu.VMEM((groups, local_experts * keep, width), bf16),
            dma((6,)),
            dma((3 * local_experts,)),
            dma((local_experts,)),
            dma((local_experts,)),
            dma((3,)),
            dma((3,)),
            dma((groups - 1,)),
            dma((groups - 1,)),
            dma((3 * members,)),
            dma((3 * members,)),
            dma((3 * members + 1,)),
            dma((3 * members + 1,)),
            dma((8,)),
            dma((8,)),
            dma((members - 1,)),
            dma((members - 1,)),
        ],
        compiler_params=pltpu.CompilerParams(
            collective_id=0, has_side_effects=True, vmem_limit_bytes=58 * 1024 * 1024
        ),
    )(inputs, gates, tokens, gain, gate_t, up_t, w_down, residual, w_qkv)


def out_kernel(stream_ref, projected_ref, stream_hbm, projected_hbm, sem):
    copies = [
        pltpu.make_async_copy(projected_ref, projected_hbm, sem.at[0]),
        pltpu.make_async_copy(stream_ref, stream_hbm, sem.at[1]),
    ]
    for copy in copies:
        copy.start()
    for copy in copies:
        copy.wait()


def put_out(stream, projected):
    return pl.pallas_call(
        out_kernel,
        in_specs=[pl.BlockSpec(memory_space=pltpu.VMEM)] * 2,
        out_specs=[pl.BlockSpec(memory_space=pltpu.HBM)] * 2,
        out_shape=[jax.ShapeDtypeStruct(v.shape, v.dtype) for v in (stream, projected)],
        scratch_shapes=[pltpu.SemaphoreType.DMA((2,))],
        compiler_params=pltpu.CompilerParams(vmem_limit_bytes=8 * 1024 * 1024),
    )(stream, projected)


def plain_rows(
    expert_inputs, gates, w_gate, w_up, w_down, send_table, expert_count, tensor_count
):
    local_experts, slot_count, feature_width = expert_inputs.shape
    gate_part = jnp.einsum(
        "ecd,edf->ecf", expert_inputs, w_gate, preferred_element_type=jnp.float32
    )
    up_part = jnp.einsum("ecd,edf->ecf", expert_inputs, w_up, preferred_element_type=jnp.float32)
    hidden = (jax.nn.silu(gate_part) * up_part).astype(jnp.bfloat16)
    partial_value = (
        jnp.einsum("ecf,efd->ecd", hidden, w_down, preferred_element_type=jnp.float32)
        * gates[:, :, None]
    ).astype(jnp.bfloat16)
    row_total = local_experts * slot_count
    arrived = lax.all_to_all(
        partial_value.reshape(row_total, feature_width),
        "tensor",
        split_axis=1,
        concat_axis=0,
        tiled=True,
    ).reshape(tensor_count, local_experts, slot_count, -1)
    summed = jnp.sum(arrived.astype(jnp.float32), axis=0).astype(jnp.bfloat16)

    outgoing = jnp.einsum("zlkmj,mjf->zlkf", send_table, summed)
    incoming = lax.all_to_all(
        outgoing.reshape(expert_count, -1, outgoing.shape[-1]),
        "expert",
        split_axis=0,
        concat_axis=0,
        tiled=True,
    )
    incoming = incoming.reshape(-1, outgoing.shape[-1])
    return lax.all_gather(incoming, "tensor", axis=0, tiled=False)


def per_device(
    expert_inputs, gates, chosen_tokens, w_gate, w_up, w_down, residual, norm_gain, w_qkv
):
    expert_count = lax.axis_size("expert")
    tensor_count = lax.axis_size("tensor")
    my_group = lax.axis_index("expert")
    local_experts, slot_count, feature_width = expert_inputs.shape
    tok_rows = residual.shape[0]
    group_rows = tok_rows * tensor_count
    keep = min(slot_count, MOST * tensor_count)
    if tensor_count == 8:
        return put_out(
            *communicate(
                expert_count,
                tensor_count,
                keep,
                expert_inputs,
                gates,
                chosen_tokens,
                w_gate,
                w_up,
                w_down,
                residual,
                norm_gain[None, :],
                w_qkv,
            )
        )

    dest = chosen_tokens // group_rows
    earlier = jnp.arange(slot_count)[None, :] < jnp.arange(slot_count)[:, None]
    rank = jnp.sum(
        ((dest[:, :, None] == dest[:, None, :]) & earlier[None]).astype(jnp.int32), axis=2
    )
    kept = jnp.arange(keep, dtype=jnp.int32)
    mine = jnp.where(dest == my_group, rank, -1)
    token_at = jnp.sum(
        jnp.where(
            mine[:, None, :] == kept[None, :, None],
            (chosen_tokens % group_rows)[:, None, :] + 1,
            0,
        ),
        axis=2,
    ).reshape(1, -1) - 1

    local_dest = lax.dynamic_slice_in_dim(dest, my_group * local_experts, local_experts, 0)
    local_rank = lax.dynamic_slice_in_dim(rank, my_group * local_experts, local_experts, 0)
    send_table = (
        (local_dest[None, :, None, :] == jnp.arange(expert_count)[:, None, None, None])
        & (local_rank[None, :, None, :] == kept[None, None, :, None])
    ).astype(jnp.bfloat16)
    same = jnp.eye(local_experts, dtype=jnp.bfloat16)
    send_table = send_table[:, :, :, None, :] * same[None, :, None, :, None]
    residual_all = lax.all_gather(residual, "tensor", axis=0, tiled=True)
    rows = plain_rows(
        expert_inputs, gates, w_gate, w_up, w_down, send_table, expert_count, tensor_count
    )
    order = tuple(range(tensor_count))
    return finish(
        lax.axis_index("tensor").reshape(1),
        token_at,
        residual_all,
        rows,
        order,
        norm_gain[None, :],
        w_qkv,
        tok_rows,
    )


def solution(mesh):
    return jax.shard_map(
        per_device,
        mesh=mesh,
        in_specs=(
            P("expert", None, None),
            P("expert", None),
            P(),
            P("expert", None, "tensor"),
            P("expert", None, "tensor"),
            P("expert", "tensor", None),
            P(("expert", "tensor"), None),
            P(),
            P(None, "tensor"),
        ),
        out_specs=(P(("expert", "tensor"), None), P("expert", "tensor")),
        check_vma=False,
    )
```

```python
import functools

import jax
import jax.numpy as jnp
from jax import lax
from jax.experimental import pallas as pl
from jax.experimental.pallas import tpu as pltpu
from jax.sharding import PartitionSpec as P

MOST = 4
MESH = pl.DeviceIdType.MESH


def finish_kernel(
    row_steps,
    order,
    owner_ref,
    slots_ref,
    residual_ref,
    rows_ref,
    gain_ref,
    weight_ref,
    stream_ref,
    projected_ref,
    combined_ref,
    normed_ref,
):
    step = pl.program_id(0)
    tok_rows, feature_width = residual_ref.shape
    chunk = rows_ref.shape[2]

    @pl.when(step < row_steps)
    def _():
        tokens = lax.broadcasted_iota(jnp.int32, (tok_rows, slots_ref.shape[1]), 0)
        placement = jnp.where(slots_ref[...] == tokens + step * tok_rows, 1.0, 0.0).astype(
            jnp.bfloat16
        )
        squares = jnp.zeros((tok_rows, 128), jnp.float32)
        for place, start in enumerate(range(0, feature_width, chunk)):
            cols = pl.ds(start, chunk)
            combined = residual_ref[:, cols].astype(jnp.float32) + jnp.dot(
                placement, rows_ref[order[place]], preferred_element_type=jnp.float32
            )
            combined_ref[:, cols] = combined
            for part in range(0, chunk, 128):
                piece = combined[:, part : part + 128]
                squares = squares + piece * piece
        mean = jnp.sum(squares, axis=1, keepdims=True) / feature_width
        scale = lax.rsqrt(mean + 1e-06)
        begin = pl.multiple_of(step * tok_rows, tok_rows)
        for start in range(0, feature_width, chunk):
            cols = pl.ds(start, chunk)
            normed_ref[pl.ds(begin, tok_rows), cols] = (
                combined_ref[:, cols] * scale * gain_ref[:, cols]
            ).astype(jnp.bfloat16)

        @pl.when(step == owner_ref[0])
        def _():
            stream_ref[...] = combined_ref[...].astype(jnp.bfloat16)

    @pl.when(step >= row_steps)
    def _():
        projected_ref[...] = jnp.dot(
            normed_ref[...], weight_ref[...], preferred_element_type=jnp.float32
        ).astype(jnp.bfloat16)


def finish(owner, slots, residual_all, rows, order, gain, w_qkv, tok_rows):
    total_rows, feature_width = residual_all.shape
    columns = w_qkv.shape[1]
    tile = 256
    row_steps = total_rows // tok_rows
    col_steps = columns // tile
    slot_total = rows.shape[1]
    return pl.pallas_call(
        functools.partial(finish_kernel, row_steps, order),
        grid=(row_steps + col_steps,),
        in_specs=[
            pl.BlockSpec(memory_space=pltpu.SMEM),
            pl.BlockSpec((1, slot_total), lambda i: (0, 0)),
            pl.BlockSpec((tok_rows, feature_width), lambda i: (jnp.minimum(i, row_steps - 1), 0)),
            pl.BlockSpec(rows.shape, lambda i: (0, 0, 0)),
            pl.BlockSpec((1, feature_width), lambda i: (0, 0)),
            pl.BlockSpec((feature_width, tile), lambda i: (0, jnp.maximum(i - row_steps, 0))),
        ],
        out_specs=[
            pl.BlockSpec((tok_rows, feature_width), lambda i: (0, 0)),
            pl.BlockSpec((total_rows, tile), lambda i: (0, jnp.maximum(i - row_steps, 0))),
        ],
        out_shape=[
            jax.ShapeDtypeStruct((tok_rows, feature_width), jnp.bfloat16),
            jax.ShapeDtypeStruct((total_rows, columns), jnp.bfloat16),
        ],
        scratch_shapes=[
            pltpu.VMEM((tok_rows, feature_width), jnp.float32),
            pltpu.VMEM((total_rows, feature_width), jnp.bfloat16),
        ],
        compiler_params=pltpu.CompilerParams(
            vmem_limit_bytes=60 * 1024 * 1024, dimension_semantics=("arbitrary",)
        ),
        cost_estimate=pl.CostEstimate(
            flops=2 * total_rows * feature_width * (columns + slot_total),
            bytes_accessed=2 * (feature_width * columns + total_rows * columns),
            transcendentals=0,
        ),
    )(owner, slots, residual_all, rows, gain, w_qkv)


def comm_kernel(
    groups,
    keep,
    inputs_hbm,
    gates_hbm,
    tokens_hbm,
    gain_hbm,
    gate_hbm,
    up_hbm,
    down_hbm,
    residual_hbm,
    weight_hbm,
    stream_ref,
    projected_ref,
    inputs,
    gates,
    tokens,
    gain,
    gate_w,
    up_w,
    down_w,
    raw,
    weight,
    blocks,
    rows,
    acc,
    row_acc,
    row_out,
    ranks,
    slot_col,
    slots,
    scales,
    partial,
    half_in,
    chips_sum,
    chips_in,
    outgoing,
    squares,
    own_place,
    scale_cols,
    load_sem,
    expert_sem,
    first_send,
    first_recv,
    reduce_send,
    reduce_recv,
    group_send,
    group_recv,
    link_send,
    link_recv,
    pair_send,
    pair_recv,
    row_send,
    row_recv,
    scale_send,
    scale_recv,
):
    group = lax.axis_index("expert")
    me = lax.axis_index("tensor")
    core = me % 2
    partner = me + 1 - 2 * core
    along_x = me + 2 - 4 * ((me // 2) % 2)
    along_y = me + 4 - 8 * (me // 4)
    across = along_x + 4 - 8 * (me // 4)
    local_experts, slot_count, feature_width = inputs.shape
    chips, row_total, width = chips_sum.shape
    members, units, tok_rows, _ = blocks.shape
    pair = 2 * tok_rows
    half_units = units // 2
    group_rows = members * tok_rows
    slot_total = slots.shape[1]
    tile = 512
    col_tiles = weight.shape[1] // tile
    f32, bf16 = jnp.float32, jnp.bfloat16

    def load(source, target, sem):
        copy = pltpu.make_async_copy(source, target, sem)
        copy.start()
        return copy

    load_tokens = load(tokens_hbm, tokens, load_sem.at[0])
    load_gates = load(gates_hbm, gates, load_sem.at[1])
    load_gain = load(gain_hbm, gain, load_sem.at[2])
    load_raw = load(residual_hbm, raw, load_sem.at[3])
    load_inputs = load(inputs_hbm, inputs, load_sem.at[4])

    def load_expert(expert):
        return [
            load(hbm.at[expert], vmem.at[expert], expert_sem.at[3 * expert + index])
            for index, (hbm, vmem) in enumerate(
                ((gate_hbm, gate_w), (up_hbm, up_w), (down_hbm, down_w))
            )
        ]

    load_experts = [load_expert(0)]

    barrier = pltpu.get_barrier_semaphore()
    peers = [(group, lax.rem(me + d, members)) for d in range(1, members)]
    peers += [((group + d) % groups, me) for d in range(1, groups)]
    for device in peers:
        pl.semaphore_signal(barrier, inc=1, device_id=device, device_id_type=MESH)

    def settle(ref, sem):
        pltpu.make_async_copy(ref, ref, sem).wait()

    def send(source, target, send_sem, recv_sem, device):
        copy = pltpu.make_async_remote_copy(
            src_ref=source,
            dst_ref=target,
            send_sem=send_sem,
            recv_sem=recv_sem,
            device_id=(group, device),
            device_id_type=MESH,
        )
        copy.start()
        return copy

    half_rows = tok_rows // 2

    def on_link(kind, index, origin, unit, device):
        part = blocks.at[origin, unit]
        send(part, part, link_send.at[kind], link_recv.at[index], device)

    def own_pair(index, unit_x, unit_y):
        on_link(0, index, me, unit_x, along_x)
        on_link(1, index, me, unit_y, along_y)

    def relay_pair(step):
        on_link(2, units + step, along_x, step, along_y)
        on_link(2, units + step, along_y, half_units + step, along_x)

    def own_ends():
        for side in range(2):
            for kind, unit, device in ((0, units - 1, along_x), (1, half_units - 1, along_y)):
                part = blocks.at[me, unit, pl.ds(side * half_rows, half_rows)]
                send(
                    part,
                    part,
                    link_send.at[kind],
                    link_recv.at[units + half_units + side],
                    device,
                )

    def to_partner(index, role, unit, start=0, size=tok_rows):
        part = blocks.at[(along_x, along_y, across)[role], unit, pl.ds(start, size)]
        send(part, part, pair_send.at[role], pair_recv.at[index], partner)

    two_units = blocks.at[me, pl.ds(0, 2)]
    one_unit = blocks.at[me, 0]

    def rows_to(index, origin, start, size, device):
        part = rows.at[origin, pl.ds(start, size)]
        return send(part, part, row_send, row_recv.at[index], device)

    def eye(size):
        shape = (size, size)
        return lax.broadcasted_iota(jnp.int32, shape, 0) == lax.broadcasted_iota(
            jnp.int32, shape, 1
        )

    def column(row):
        return jnp.sum(jnp.where(eye(row.shape[1]), row, 0.0), axis=1, keepdims=True)

    load_tokens.wait()
    order = lax.broadcasted_iota(jnp.int32, (slot_count, slot_count), 0)
    later = lax.broadcasted_iota(jnp.int32, (slot_count, slot_count), 1)
    before = jnp.where(order < later, 1.0, 0.0).astype(bf16)
    chosen = tokens[...]
    for place in range(groups):
        inside = (chosen >= place * group_rows) & (chosen < (place + 1) * group_rows)
        taken = jnp.where(inside, 1.0, 0.0)
        rank = jnp.dot(taken.astype(bf16), before, preferred_element_type=f32)
        ranks[place] = jnp.where(inside, rank, -1.0)
    kept = lax.broadcasted_iota(jnp.int32, (keep, slot_count), 0).astype(f32)
    mine = ranks[group]
    local = (chosen - group * group_rows + 1).astype(f32)
    for expert in range(chosen.shape[0]):
        hit = mine[expert : expert + 1, :] == kept
        slot_col[expert * keep : (expert + 1) * keep, :] = jnp.sum(
            jnp.where(hit, local[expert : expert + 1, :], 0.0), axis=1, keepdims=True
        )
    slots[...] = (
        jnp.sum(jnp.where(eye(slot_total), slot_col[...], 0.0), axis=0, keepdims=True) - 1.0
    )

    load_gain.wait()
    load_raw.wait()
    load_experts += [load_expert(expert) for expert in range(1, local_experts)]
    for unit in range(units):
        cols = pl.ds(unit * width, width)
        blocks[me, unit] = (raw[:, cols].astype(f32) * gain[:, cols]).astype(bf16)

    pl.semaphore_wait(barrier, len(peers))

    own_pair(0, 0, half_units)
    own_pair(1, 1, half_units + 1)
    own_pair(2, 2, half_units + 2)
    part = blocks.at[me]
    send(part, part, pair_send.at[3], pair_recv.at[units + half_units + 2], partner)

    load_gates.wait()
    load_inputs.wait()
    contract = (((1,), (1,)), ((), ()))
    firsts = []
    for expert in range(local_experts):
        for copy in load_experts[expert]:
            copy.wait()
        if expert == 0:
            load_weight = load(weight_hbm, weight, load_sem.at[5])
        gate_part = lax.dot_general(
            inputs[expert], gate_w[expert], contract, preferred_element_type=f32
        )
        up_part = lax.dot_general(
            inputs[expert], up_w[expert], contract, preferred_element_type=f32
        )
        hidden = (gate_part / (1.0 + jnp.exp(-gate_part)) * up_part).astype(bf16)
        scale_by = column(gates[expert : expert + 1, :])
        lines = pl.ds(expert * slot_count, slot_count)
        for place in range(2 * chips):
            value = jnp.dot(
                hidden,
                down_w[expert, :, place * width : (place + 1) * width],
                preferred_element_type=f32,
            )
            partial[place, lines, :] = (value * scale_by).astype(bf16)
        firsts.append(
            send(
                partial.at[pl.ds((1 - core) * chips, chips), lines],
                half_in.at[:, lines],
                first_send,
                first_recv.at[expert],
                partner,
            )
        )

    for expert, copy in enumerate(firsts):
        copy.wait_recv()
        lines = pl.ds(expert * slot_count, slot_count)
        for chip in range(chips):
            chips_sum[chip, lines, :] = (
                partial[core * chips + chip, lines, :].astype(f32)
                + half_in[chip, lines, :].astype(f32)
            ).astype(bf16)
    for index, device in enumerate((across, along_x, along_y)):
        send(chips_sum.at[device // 2], chips_in.at[index], reduce_send, reduce_recv, device)
    own_pair(3, 3, half_units + 3)

    def product(chip, unit, index):
        lines = pl.ds(pl.multiple_of(unit * width, width), width)
        left = blocks[pl.ds(2 * chip, 2), unit].reshape(pair, width)
        cols = pl.ds(index * tile, tile)
        return jnp.dot(left, weight[lines, cols], preferred_element_type=f32)

    def accumulate(chip, unit):
        for index in range(col_tiles):
            acc[chip, :, pl.ds(index * tile, tile)] += product(chip, unit, index)

    def clear(chip, carry):
        acc[chip] = jnp.zeros(acc.shape[1:], f32)
        return carry

    lax.fori_loop(0, chips, clear, 0)
    row_acc[...] = jnp.zeros(row_acc.shape, f32)
    squares[...] = jnp.zeros(squares.shape, f32)

    chip_own, chip_x, chip_y, chip_a = me // 2, along_x // 2, along_y // 2, across // 2

    def each(start, size, body):
        def step(index, carry):
            body(index)
            return carry

        lax.fori_loop(start, start + size, step, 0)

    def own(index):
        accumulate(chip_own, index)
        accumulate(chip_own, index + half_units)

    def near(index):
        accumulate(chip_x, index)
        accumulate(chip_y, index + half_units)

    def late(index):
        accumulate(chip_x, index + half_units)
        accumulate(chip_y, index)

    def far(index):
        accumulate(chip_a, index)
        accumulate(chip_a, index + half_units)

    def forward(step):
        settle(two_units, link_recv.at[step])
        to_partner(step, 0, step)
        to_partner(step, 1, half_units + step)

    def forward_late(step):
        settle(two_units, link_recv.at[half_units + step])
        to_partner(half_units + step, 0, half_units + step)
        to_partner(half_units + step, 1, step)

    def forward_far(step):
        settle(two_units, link_recv.at[units + step])
        to_partner(units + step, 2, step)
        to_partner(units + step, 2, half_units + step)

    def arrive(kind, step):
        settle(two_units, pair_recv.at[{"near": 0, "late": half_units, "far": units}[kind] + step])

    forward(0)
    forward(1)
    relay_pair(0)
    relay_pair(1)
    settle(blocks.at[me], pair_recv.at[units + half_units + 2])
    load_weight.wait()
    each(0, half_units, own)
    arrive("near", 0)
    arrive("near", 1)
    each(0, 2, near)

    settle(chips_in, reduce_recv)
    total = chips_sum[me // 2].astype(f32)
    for index in range(3):
        total = total + chips_in[index].astype(f32)
    total = total.astype(bf16)
    for place in range(groups):
        for expert in range(local_experts):
            rank = ranks[place, pl.ds(group * local_experts + expert, 1), :]
            table = jnp.where(rank == kept, 1.0, 0.0).astype(bf16)
            outgoing[place, expert * keep : (expert + 1) * keep, :] = jnp.dot(
                table,
                total[expert * slot_count : (expert + 1) * slot_count],
                preferred_element_type=f32,
            ).astype(bf16)
    for d in range(1, groups):
        pltpu.make_async_remote_copy(
            src_ref=outgoing.at[(group + d) % groups],
            dst_ref=rows.at[me, group],
            send_sem=group_send,
            recv_sem=group_recv,
            device_id=((group + d) % groups, me),
            device_id_type=MESH,
        ).start()
    rows[me, group] = outgoing[group]

    forward(2)
    arrive("near", 2)
    each(2, 1, near)
    forward(3)
    arrive("near", 3)
    each(3, 1, near)

    settle(outgoing.at[pl.ds(0, groups - 1)], group_recv)
    groups_half = groups // 2
    rest = groups - groups_half
    row_x, row_y = rows_to(0, me, 0, groups, along_x), rows_to(1, me, 0, groups, along_y)
    row_own = rows_to(4, me, 0, groups, partner)
    relay_pair(2)
    forward_far(0)
    forward_far(1)

    def placement(begin, size):
        line = lax.broadcasted_iota(jnp.int32, (size, slot_total), 0) + begin
        return jnp.where(slots[...] == line.astype(f32), 1.0, 0.0).astype(bf16)

    own_place[...] = placement(me * tok_rows, tok_rows)

    def take_rows(source):
        start = ((source % 2) * chips + source // 2) * width
        part = pl.ds(pl.multiple_of(start, width), width)
        values = rows[source].reshape(slot_total, width)
        combined = raw[:, part].astype(f32) + jnp.dot(
            own_place[...], values, preferred_element_type=f32
        )
        stream_ref[:, part] = combined.astype(bf16)
        total = squares[...]
        for piece in range(0, width, 128):
            value = combined[:, piece : piece + 128]
            total = total + value * value
        squares[...] = total
        values = (values.astype(f32) * gain[:, part]).astype(bf16)
        for index in range(col_tiles):
            cols = pl.ds(index * tile, tile)
            row_acc[:, cols] += jnp.dot(values, weight[part, cols], preferred_element_type=f32)

    def take_pair(chip):
        each(2 * chip, 2, take_rows)

    row_own.wait_recv()
    take_pair(chip_own)
    arrive("far", 0)
    arrive("far", 1)
    each(0, 2, far)

    row_x.wait_recv()
    row_ox = rows_to(2, along_x, 0, groups_half, along_y)
    row_px = rows_to(5, along_x, 0, groups, partner)
    row_y.wait_recv()
    row_oy = rows_to(3, along_y, groups_half, rest, along_x)
    row_py = rows_to(6, along_y, 0, groups, partner)
    relay_pair(3)
    own_pair(half_units, half_units, 0)
    row_px.wait_recv()
    take_pair(chip_x)
    row_py.wait_recv()
    take_pair(chip_y)
    forward_far(2)
    row_ox.wait_recv()
    row_oy.wait_recv()
    row_pa = rows_to(7, across, 0, groups, partner)
    own_pair(half_units + 1, half_units + 1, 1)
    arrive("far", 2)
    each(2, 1, far)
    row_pa.wait_recv()
    take_pair(chip_a)

    scale = lax.rsqrt(jnp.sum(squares[...], axis=1, keepdims=True) / feature_width + 1e-06)
    scale_row = jnp.sum(jnp.where(eye(tok_rows), scale, 0.0), axis=0, keepdims=True)
    scales[me] = jnp.broadcast_to(scale_row, scales.shape[1:])
    part = scales.at[me]
    for d in range(1, members):
        send(part, part, scale_send, scale_recv, lax.rem(me + d, members))
    own_pair(half_units + 2, half_units + 2, 2)
    own_ends()

    row_out[...] = row_acc[...].astype(bf16)

    def place_rows(chip):
        spread = placement(chip * pair, pair)
        for index in range(col_tiles):
            cols = pl.ds(index * tile, tile)
            acc[chip, :, cols] += jnp.dot(spread, row_out[:, cols], preferred_element_type=f32)

    forward_far(3)
    each(0, chips, place_rows)
    arrive("far", 3)
    each(3, 1, far)
    forward_late(0)
    arrive("late", 0)
    each(0, 1, late)
    forward_late(1)
    arrive("late", 1)
    each(1, 1, late)

    def finish(chip):
        def body(side, carry):
            lines = pl.ds(pl.multiple_of(side * tok_rows, tok_rows), tok_rows)
            begin = pl.multiple_of((2 * chip + side) * tok_rows, tok_rows)
            projected_ref[pl.ds(begin, tok_rows), :] = (
                acc[chip, lines, :] * scale_cols[2 * chip + side]
            ).astype(bf16)
            return carry

        lax.fori_loop(0, 2, body, 0)

    def close(chip, unit, start):
        first = pl.multiple_of(2 * chip * tok_rows + start, half_rows)
        left = blocks[pl.ds(2 * chip, 2), unit, pl.ds(start, half_rows), :].reshape(
            tok_rows, width
        )
        lines = pl.ds(unit * width, width)
        for index in range(col_tiles):
            cols = pl.ds(index * tile, tile)
            value = jnp.dot(left, weight[lines, cols], preferred_element_type=f32)
            for side in range(2):
                rows_in = pl.ds(side * tok_rows + start, half_rows)
                piece = value[side * half_rows : (side + 1) * half_rows]
                piece = (acc[chip, rows_in, cols] + piece) * scale_cols[
                    2 * chip + side, pl.ds(start, half_rows), :
                ]
                projected_ref[pl.ds(first + side * tok_rows, half_rows), cols] = piece.astype(
                    bf16
                )

    forward_late(2)
    settle(scales.at[pl.ds(0, members - 1)], scale_recv)

    def turn(source):
        scale_cols[source] = column(scales[source, 0:1, :])

    each(0, members, turn)
    finish(chip_own)
    finish(chip_a)
    arrive("late", 2)
    each(2, 1, late)
    settle(half_in, first_send)
    settle(chips_in, reduce_send)
    settle(outgoing.at[pl.ds(0, groups - 1)], group_send)
    settle(rows.at[pl.ds(0, 7)], row_send)
    settle(scales.at[pl.ds(0, members - 1)], scale_send)
    settle(blocks.at[me], link_send.at[2])
    for role in (2, 3):
        settle(blocks.at[me], pair_send.at[role])

    for side in range(2):
        settle(one_unit, link_recv.at[units + half_units + side])
        for role, unit in enumerate((units - 1, half_units - 1)):
            to_partner(units + half_units + side, role, unit, side * half_rows, half_rows)
    for side in range(2):
        settle(one_unit, pair_recv.at[units + half_units + side])
        close(chip_x, units - 1, side * half_rows)
        close(chip_y, half_units - 1, side * half_rows)
    for role in range(2):
        settle(blocks.at[me], link_send.at[role])
        settle(blocks.at[me], pair_send.at[role])


def communicate(
    groups, members, keep, inputs, gates, tokens, w_gate, w_up, w_down, residual, gain, w_qkv
):
    local_experts, slot_count, feature_width = inputs.shape
    tok_rows = residual.shape[0]
    row_total = local_experts * slot_count
    width = feature_width // members
    chips = members // 2
    units = members
    columns = w_qkv.shape[1]
    slot_total = tokens.shape[0] * keep
    bf16, f32 = jnp.bfloat16, jnp.float32
    hbm = pl.BlockSpec(memory_space=pltpu.HBM)
    vmem = pl.BlockSpec(memory_space=pltpu.VMEM)
    dma = pltpu.SemaphoreType.DMA
    gate_t, up_t = jnp.swapaxes(w_gate, 1, 2), jnp.swapaxes(w_up, 1, 2)
    return pl.pallas_call(
        functools.partial(comm_kernel, groups, keep),
        in_specs=[hbm] * 9,
        out_specs=[vmem, vmem],
        out_shape=[
            pltpu.VMEM((tok_rows, feature_width), bf16),
            pltpu.VMEM((members * tok_rows, columns), bf16),
        ],
        scratch_shapes=[
            pltpu.VMEM(inputs.shape, bf16),
            pltpu.VMEM(gates.shape, f32),
            pltpu.VMEM(tokens.shape, jnp.int32),
            pltpu.VMEM(gain.shape, f32),
            pltpu.VMEM(gate_t.shape, bf16),
            pltpu.VMEM(up_t.shape, bf16),
            pltpu.VMEM(w_down.shape, bf16),
            pltpu.VMEM(residual.shape, bf16),
            pltpu.VMEM(w_qkv.shape, bf16),
            pltpu.VMEM((members, members, tok_rows, width), bf16),
            pltpu.VMEM((members, groups, local_experts * keep, width), bf16),
            pltpu.VMEM((chips, 2 * tok_rows, columns), f32),
            pltpu.VMEM((slot_total, columns), f32),
            pltpu.VMEM((slot_total, columns), bf16),
            pltpu.VMEM((groups,) + tokens.shape, f32),
            pltpu.VMEM((slot_total, 1), f32),
            pltpu.VMEM((1, slot_total), f32),
            pltpu.VMEM((members, 8, tok_rows), f32),
            pltpu.VMEM((members, row_total, width), bf16),
            pltpu.VMEM((chips, row_total, width), bf16),
            pltpu.VMEM((chips, row_total, width), bf16),
            pltpu.VMEM((chips - 1, row_total, width), bf16),
            pltpu.VMEM((groups, local_experts * keep, width), bf16),
            pltpu.VMEM((tok_rows, 128), f32),
            pltpu.VMEM((tok_rows, slot_total), bf16),
            pltpu.VMEM((members, tok_rows, 1), f32),
            dma((6,)),
            dma((3 * local_experts,)),
            dma,
            dma((local_experts,)),
            dma,
            dma,
            dma,
            dma,
            dma((3,)),
            dma((units + units // 2 + 2,)),
            dma((4,)),
            dma((units + units // 2 + 3,)),
            dma,
            dma((8,)),
            dma,
            dma,
        ],
        compiler_params=pltpu.CompilerParams(
            collective_id=0, has_side_effects=True, vmem_limit_bytes=58 * 1024 * 1024
        ),
    )(inputs, gates, tokens, gain, gate_t, up_t, w_down, residual, w_qkv)


def out_kernel(stream_ref, projected_ref, stream_hbm, projected_hbm, sem):
    copies = [
        pltpu.make_async_copy(projected_ref, projected_hbm, sem.at[0]),
        pltpu.make_async_copy(stream_ref, stream_hbm, sem.at[1]),
    ]
    for copy in copies:
        copy.start()
    for copy in copies:
        copy.wait()


def put_out(stream, projected):
    return pl.pallas_call(
        out_kernel,
        in_specs=[pl.BlockSpec(memory_space=pltpu.VMEM)] * 2,
        out_specs=[pl.BlockSpec(memory_space=pltpu.HBM)] * 2,
        out_shape=[jax.ShapeDtypeStruct(v.shape, v.dtype) for v in (stream, projected)],
        scratch_shapes=[pltpu.SemaphoreType.DMA((2,))],
        compiler_params=pltpu.CompilerParams(vmem_limit_bytes=8 * 1024 * 1024),
    )(stream, projected)


def plain_rows(
    expert_inputs, gates, w_gate, w_up, w_down, send_table, expert_count, tensor_count
):
    local_experts, slot_count, feature_width = expert_inputs.shape
    gate_part = jnp.einsum(
        "ecd,edf->ecf", expert_inputs, w_gate, preferred_element_type=jnp.float32
    )
    up_part = jnp.einsum("ecd,edf->ecf", expert_inputs, w_up, preferred_element_type=jnp.float32)
    hidden = (jax.nn.silu(gate_part) * up_part).astype(jnp.bfloat16)
    partial_value = (
        jnp.einsum("ecf,efd->ecd", hidden, w_down, preferred_element_type=jnp.float32)
        * gates[:, :, None]
    ).astype(jnp.bfloat16)
    row_total = local_experts * slot_count
    arrived = lax.all_to_all(
        partial_value.reshape(row_total, feature_width),
        "tensor",
        split_axis=1,
        concat_axis=0,
        tiled=True,
    ).reshape(tensor_count, local_experts, slot_count, -1)
    summed = jnp.sum(arrived.astype(jnp.float32), axis=0).astype(jnp.bfloat16)

    outgoing = jnp.einsum("zlkmj,mjf->zlkf", send_table, summed)
    incoming = lax.all_to_all(
        outgoing.reshape(expert_count, -1, outgoing.shape[-1]),
        "expert",
        split_axis=0,
        concat_axis=0,
        tiled=True,
    )
    incoming = incoming.reshape(-1, outgoing.shape[-1])
    return lax.all_gather(incoming, "tensor", axis=0, tiled=False)


def per_device(
    expert_inputs, gates, chosen_tokens, w_gate, w_up, w_down, residual, norm_gain, w_qkv
):
    expert_count = lax.axis_size("expert")
    tensor_count = lax.axis_size("tensor")
    my_group = lax.axis_index("expert")
    local_experts, slot_count, feature_width = expert_inputs.shape
    tok_rows = residual.shape[0]
    group_rows = tok_rows * tensor_count
    keep = min(slot_count, MOST * tensor_count)
    if tensor_count == 8:
        return put_out(
            *communicate(
                expert_count,
                tensor_count,
                keep,
                expert_inputs,
                gates,
                chosen_tokens,
                w_gate,
                w_up,
                w_down,
                residual,
                norm_gain[None, :],
                w_qkv,
            )
        )

    dest = chosen_tokens // group_rows
    earlier = jnp.arange(slot_count)[None, :] < jnp.arange(slot_count)[:, None]
    rank = jnp.sum(
        ((dest[:, :, None] == dest[:, None, :]) & earlier[None]).astype(jnp.int32), axis=2
    )
    kept = jnp.arange(keep, dtype=jnp.int32)
    mine = jnp.where(dest == my_group, rank, -1)
    token_at = jnp.sum(
        jnp.where(
            mine[:, None, :] == kept[None, :, None],
            (chosen_tokens % group_rows)[:, None, :] + 1,
            0,
        ),
        axis=2,
    ).reshape(1, -1) - 1

    local_dest = lax.dynamic_slice_in_dim(dest, my_group * local_experts, local_experts, 0)
    local_rank = lax.dynamic_slice_in_dim(rank, my_group * local_experts, local_experts, 0)
    send_table = (
        (local_dest[None, :, None, :] == jnp.arange(expert_count)[:, None, None, None])
        & (local_rank[None, :, None, :] == kept[None, None, :, None])
    ).astype(jnp.bfloat16)
    same = jnp.eye(local_experts, dtype=jnp.bfloat16)
    send_table = send_table[:, :, :, None, :] * same[None, :, None, :, None]
    residual_all = lax.all_gather(residual, "tensor", axis=0, tiled=True)
    rows = plain_rows(
        expert_inputs, gates, w_gate, w_up, w_down, send_table, expert_count, tensor_count
    )
    order = tuple(range(tensor_count))
    return finish(
        lax.axis_index("tensor").reshape(1),
        token_at,
        residual_all,
        rows,
        order,
        norm_gain[None, :],
        w_qkv,
        tok_rows,
    )


def solution(mesh):
    return jax.shard_map(
        per_device,
        mesh=mesh,
        in_specs=(
            P("expert", None, None),
            P("expert", None),
            P(),
            P("expert", None, "tensor"),
            P("expert", None, "tensor"),
            P("expert", "tensor", None),
            P(("expert", "tensor"), None),
            P(),
            P(None, "tensor"),
        ),
        out_specs=(P(("expert", "tensor"), None), P("expert", "tensor")),
        check_vma=False,
    )
```
